16 devices in a mesh: dp: 4 (over y, z, core), sp: 4 (over x).
Axes of the slice: x: 4, y: 2, z: 1, core: 2. Of those that a mesh axis runs over, the one named last changes fastest.
The devices are a block of a 4x4x8 slice.
Arguments:
- x: bfloat16 [8192, 8192], P(('dp', 'sp')), parts along dimension 0
- gain: bfloat16 [8192], replicated
- wq: bfloat16 [8192, 8192], replicated
- wk: bfloat16 [8192, 1024], replicated
- wv: bfloat16 [8192, 1024], replicated
- wo: bfloat16 [8192, 8192], replicated
Outputs:
- output: bfloat16 [8192, 8192], P(('dp', 'sp')), parts along dimension 0
There are 4 independent parts. The reference program is written for one: setup_inputs(seed, part) draws one part's arguments, and reference() takes and returns one part's arrays. A program takes and returns all parts, laid end to end along the dimension named above; an argument that names none is the same for every part.
All inputs are finite; a program needn't handle non-finite values.
Results may differ from the reference program's by a relative error of at most 0.012.
Values are sent between devices in bfloat16 or wider.
A program may use at most 768 MiB of HBM per device.

```python
import jax
import jax.numpy as jnp
from jax import lax

ROWS = 2048
D = 8192
HEADS = 64
KV_HEADS = 8
HEAD = 128
THETA = 10000


def setup_inputs(seed: int = 0, part: int = 0) -> dict:
    kx, kn, kq, kk, kv, ko = jax.random.split(jax.random.key(seed), 6)

    def weights(key, rows, columns):
        return jax.random.normal(key, (rows, columns), jnp.float32) * rows**-0.5

    drawn = {
        "x": jax.random.normal(jax.random.fold_in(kx, part), (ROWS, D), jnp.float32),
        "gain": 1 + 0.1 * jax.random.normal(kn, (D,), jnp.float32),
        "wq": 2 * weights(kq, D, HEADS * HEAD),
        "wk": 2 * weights(kk, D, KV_HEADS * HEAD),
        "wv": 4 * weights(kv, D, KV_HEADS * HEAD),
        "wo": weights(ko, HEADS * HEAD, D),
    }
    return {k: v.astype(jnp.bfloat16) for k, v in drawn.items()}


def normed(x, gain):
    wide = x.astype(jnp.float32)
    scale = lax.rsqrt(jnp.mean(wide * wide, -1, keepdims=True) + 1e-6)
    return (wide * scale * gain.astype(jnp.float32)).astype(jnp.bfloat16)


def turned(t, place, theta):
    half = t.shape[-1] // 2
    angle = place.astype(jnp.float32)[:, None] * theta ** (-jnp.arange(half, dtype=jnp.float32) / half)
    cos, sin = jnp.cos(angle)[:, None], jnp.sin(angle)[:, None]
    a, b = t[..., :half].astype(jnp.float32), t[..., half:].astype(jnp.float32)
    return jnp.concatenate([a * cos - b * sin, b * cos + a * sin], -1).astype(jnp.bfloat16)


def matmul(a, w):
    return jnp.dot(a, w, preferred_element_type=jnp.float32).astype(jnp.bfloat16)


def einsum(form, a, b):
    return jnp.einsum(form, a.astype(jnp.float32), b.astype(jnp.float32))


def attention(q, k, v):
    scores = einsum("tgsd,ugd->gstu", q, k) * q.shape[-1] ** -0.5
    token = jnp.arange(q.shape[0])
    scores = jnp.where(token[:, None] >= token, scores, -jnp.inf)
    weights = jax.nn.softmax(scores, -1).astype(jnp.bfloat16)
    return einsum("gstu,ugd->tgsd", weights, v).astype(jnp.bfloat16)


def reference(x, gain, wq, wk, wv, wo):
    a, place = normed(x, gain), jnp.arange(ROWS)
    q = turned(matmul(a, wq).reshape(ROWS, HEADS, HEAD), place, THETA).reshape(ROWS, KV_HEADS, -1, HEAD)
    k = turned(matmul(a, wk).reshape(ROWS, KV_HEADS, HEAD), place, THETA)
    v = matmul(a, wv).reshape(ROWS, KV_HEADS, HEAD)
    seen = attention(q, k, v).reshape(ROWS, HEADS * HEAD)
    return (x.astype(jnp.float32) + jnp.dot(seen, wo, preferred_element_type=jnp.float32)).astype(jnp.bfloat16)
```

```python
import functools

import jax
import jax.numpy as jnp
from jax import lax
from jax.experimental import pallas as pl
from jax.experimental.pallas import tpu as pltpu
from jax.sharding import PartitionSpec as P

HEAD = 128
THETA = 10000
NEG = -1e30
HIDDEN = 2 * NEG
LOG2E = 1.4426950408889634
VMEM = 60 * 2**20
F32, BF16 = jnp.float32, jnp.bfloat16


def _dot(a, b, ca, cb):
    return lax.dot_general(a, b, (((ca,), (cb,)), ((), ())), preferred_element_type=F32)


def _turn(acc, cos_ref, sin_ref, o_ref):
    cos, sin = cos_ref[...], sin_ref[...]
    for at in range(0, acc.shape[1], HEAD):
        t = acc[:, at : at + HEAD].astype(BF16).astype(F32)
        o_ref[:, at : at + HEAD] = (t * cos + pltpu.roll(t, HEAD // 2, 1) * sin).astype(BF16)


def _kv_kernel(nk, x_ref, gain_ref, wk_ref, wv_ref, cos_ref, sin_ref, a_ref, kv_ref):
    i = pl.program_id(0)

    @pl.when(i == 0)
    def _():
        rows = 32

        def norm(r, _):
            at = pl.ds(pl.multiple_of(r * rows, rows), rows)
            wide = x_ref[at, :].astype(F32)
            scale = lax.rsqrt(jnp.mean(wide * wide, -1, keepdims=True) + 1e-6)
            a_ref[at, :] = (wide * scale * gain_ref[...].astype(F32)).astype(BF16)

        lax.fori_loop(0, x_ref.shape[0] // rows, norm, None)

    @pl.when(i < nk)
    def _():
        _turn(_dot(a_ref[...], wk_ref[...], 1, 0), cos_ref, sin_ref, kv_ref)

    @pl.when(i >= nk)
    def _():
        kv_ref[...] = _dot(a_ref[...], wv_ref[...], 1, 0).astype(BF16)


def project_kv(x, gain, wk, wv, cos, sin, bn=512):
    m, d = x.shape
    n = wk.shape[1]
    nk, nv = n // bn, wv.shape[1] // bn
    whole = lambda i: (0, 0)
    return pl.pallas_call(
        functools.partial(_kv_kernel, nk),
        grid=(nk + nv,),
        in_specs=[
            pl.BlockSpec((m, d), whole, pipeline_mode=pl.Buffered(1)),
            pl.BlockSpec((1, d), whole),
            pl.BlockSpec((d, bn), lambda i: (0, jnp.minimum(i, nk - 1))),
            pl.BlockSpec((d, bn), lambda i: (0, jnp.maximum(i - nk, 0))),
            pl.BlockSpec((m, HEAD), whole),
            pl.BlockSpec((m, HEAD), whole),
        ],
        out_specs=[pl.BlockSpec((m, d), whole), pl.BlockSpec((m, bn), lambda i: (0, i))],
        out_shape=[jax.ShapeDtypeStruct((m, d), BF16), jax.ShapeDtypeStruct((m, n + wv.shape[1]), BF16)],
        compiler_params=pltpu.CompilerParams(vmem_limit_bytes=VMEM),
        cost_estimate=pl.CostEstimate(flops=4 * m * d * n, transcendentals=m, bytes_accessed=4 * (m * d + d * n)),
    )(x, gain.reshape(1, d), wk, wv, cos, sin)


def _q_kernel(a_ref, w_ref, cos_ref, sin_ref, o_ref):
    _turn(_dot(a_ref[...], w_ref[...], 1, 0), cos_ref, sin_ref, o_ref)


def project_q(a, w, cos, sin, bn=512):
    m, d = a.shape
    n = w.shape[1]
    whole = lambda i: (0, 0)
    return pl.pallas_call(
        _q_kernel,
        grid=(n // bn,),
        in_specs=[
            pl.BlockSpec((m, d), whole, pipeline_mode=pl.Buffered(1)),
            pl.BlockSpec((d, bn), lambda i: (0, i)),
            pl.BlockSpec((m, HEAD), whole),
            pl.BlockSpec((m, HEAD), whole),
        ],
        out_specs=pl.BlockSpec((m, bn), lambda i: (0, i)),
        out_shape=jax.ShapeDtypeStruct((m, n), BF16),
        compiler_params=pltpu.CompilerParams(vmem_limit_bytes=VMEM),
        cost_estimate=pl.CostEstimate(flops=2 * m * d * n, transcendentals=0, bytes_accessed=2 * (m * d + d * n + m * n)),
    )(a, w, cos, sin)


def _attend_kernel(at_ref, q_ref, k_ref, v_ref, o_ref, top_s, mix_s):
    own, heads = q_ref.shape[0], q_ref.shape[1] // HEAD
    e = HEAD**-0.5 * LOG2E
    top_s[...] = jnp.full(top_s.shape, NEG, F32)
    mix_s[...] = jnp.zeros(mix_s.shape, F32)

    def block(first, keys, cols, wide, masked):
        here = pl.ds(first, keys)
        k, values = k_ref[here, :], jnp.concatenate([v_ref[here, :].T, jnp.ones((8, keys), BF16)], axis=0)
        scores = [_dot(k, q_ref[cols : cols + wide, h * HEAD : (h + 1) * HEAD], 1, 1) for h in range(heads)]
        if masked:
            shape = (keys, wide)
            ok = lax.broadcasted_iota(jnp.int32, shape, 0) <= lax.broadcasted_iota(jnp.int32, shape, 1) + cols
        weights, keeps = [], []
        for h, s in enumerate(scores):
            if masked:
                s = jnp.where(ok, s, HIDDEN)
            old = top_s[h : h + 1, cols : cols + wide]
            top = jnp.maximum(old, s.max(axis=0, keepdims=True))
            top_s[h : h + 1, cols : cols + wide] = top
            weights.append(jnp.exp2((s - top) * e).astype(BF16))
            keeps.append(jnp.exp2((old - top) * e))
        for h in range(heads):
            mix_s[h, :, cols : cols + wide] = mix_s[h, :, cols : cols + wide] * keeps[h] + _dot(values, weights[h], 1, 0)

    lax.fori_loop(0, at_ref[0], lambda j, _: block(pl.multiple_of(j * own, own), own, 0, own, False), None)
    here = pl.multiple_of(at_ref[0] * own, own)
    half = own // 2
    block(here, half, 0, half, True)
    block(here, own, half, half, True)
    for h in range(heads):
        o_ref[:, h * HEAD : (h + 1) * HEAD] = (mix_s[h, :HEAD, :] * (1 / mix_s[h, HEAD : HEAD + 1, :])).T.astype(BF16)


def attend(q, kv, before):
    own, width = q.shape
    rows, groups = kv.shape[0], kv.shape[1] // (2 * HEAD)
    g = width // groups
    return pl.pallas_call(
        _attend_kernel,
        grid_spec=pltpu.PrefetchScalarGridSpec(
            num_scalar_prefetch=1,
            grid=(groups,),
            in_specs=[
                pl.BlockSpec((own, g), lambda i, _: (0, i)),
                pl.BlockSpec((rows, HEAD), lambda i, _: (0, i)),
                pl.BlockSpec((rows, HEAD), lambda i, _: (0, groups + i)),
            ],
            out_specs=pl.BlockSpec((own, g), lambda i, _: (0, i)),
            scratch_shapes=[pltpu.VMEM((g // HEAD, own), F32), pltpu.VMEM((g // HEAD, HEAD + 8, own), F32)],
        ),
        out_shape=jax.ShapeDtypeStruct(q.shape, BF16),
        compiler_params=pltpu.CompilerParams(vmem_limit_bytes=VMEM),
        cost_estimate=pl.CostEstimate(flops=4 * own * rows * width, transcendentals=own * rows * width // HEAD, bytes_accessed=4 * (q.size + kv.size)),
    )(before.reshape(1), q, kv, kv)


def tables(place):
    half = HEAD // 2
    angle = place.astype(F32)[:, None] * THETA ** (-jnp.arange(half, dtype=F32) / half)
    cos, sin = jnp.cos(angle), jnp.sin(angle)
    return jnp.concatenate([cos, cos], -1), jnp.concatenate([-sin, sin], -1)


def solution(mesh):
    def step(x, gain, wq, wk, wv, wo):
        own = x.shape[0]
        me = lax.axis_index("sp")
        cos, sin = tables(me * own + jnp.arange(own))
        a, kv = project_kv(x, gain, wk, wv, cos, sin)
        every = lax.all_gather(kv, "sp", axis=0, tiled=True)
        q = project_q(a, wq, cos, sin)
        seen = attend(q, every, me)
        y = jnp.dot(seen, wo, preferred_element_type=F32)
        return (x.astype(F32) + y).astype(BF16)

    tokens, whole = P(("dp", "sp"), None), P(None, None)
    return jax.shard_map(
        step,
        mesh=mesh,
        in_specs=(tokens, P(None), whole, whole, whole, whole),
        out_specs=tokens,
        check_vma=False,
    )
```

```python
import functools

import jax
import jax.numpy as jnp
from jax import lax
from jax.experimental import pallas as pl
from jax.experimental.pallas import tpu as pltpu
from jax.sharding import PartitionSpec as P

HEAD = 128
THETA = 10000
NEG = -1e30
HIDDEN = 2 * NEG
LOG2E = 1.4426950408889634
VMEM = 63 * 2**20
F32, BF16 = jnp.float32, jnp.bfloat16
SP = 4
SHIP = (0, 0, 1, 3)
MOST = max(SHIP)
BN = 512


def _dot(a, b, ca, cb):
    return lax.dot_general(a, b, (((ca,), (cb,)), ((), ())), preferred_element_type=F32)


def _by(me, values):
    out = jnp.int32(values[0])
    for s, v in enumerate(values[1:], 1):
        out = jnp.where(me == s, jnp.int32(v), out)
    return out


def _greet(me, others):
    barrier = pltpu.get_barrier_semaphore()
    for d in others:
        pl.semaphore_signal(barrier, inc=1, device_id={"sp": lax.rem(me + d, SP)}, device_id_type=pl.DeviceIdType.MESH)
    pl.semaphore_wait(barrier, len(others))


def _transfers(groups):
    s, whole = MOST * HEAD, groups * HEAD
    out = []
    for v in range(2):
        few, rest = (v * whole, s), (v * whole + s, whole - s)
        for src, dst, cols in ((0, 1, few), (0, 1, rest), (0, 3, rest), (1, 2, rest), (1, 2, few), (1, 0, few), (2, 3, rest), (2, 1, few), (3, 0, few)):
            out.append((src, dst, src, *cols, v))
        for src, dst, owner, cols in ((1, 2, 0, few), (3, 2, 0, rest), (2, 3, 1, rest), (1, 0, 2, few)):
            out.append((src, dst, owner, *cols, 2 + v))
    return out


def _project_kernel(x_ref, gain_ref, wk_ref, wv_ref, wq_ref, cos_ref, sin_ref, kv_ref, q_ref, ship_ref,
                    a_s, w_s, kv_s, q_s, x_sem, w_sem, kv_sem, q_sem, send_sem, recv_sem, ship_send, ship_recv):
    me = lax.axis_index("sp")
    own, depth = a_s.shape
    groups = wk_ref.shape[1] // HEAD
    nk, nq = wk_ref.shape[1] // BN, wq_ref.shape[1] // BN
    per = wq_ref.shape[1] // groups // BN
    lots = MOST * per
    parts = 4
    rows = own // parts

    def x_copy(p):
        at = pl.ds(p * rows, rows)
        return pltpu.make_async_copy(x_ref.at[at, :], a_s.at[at, :], x_sem.at[p])

    def w_copy(ref, i, slot):
        return pltpu.make_async_copy(ref.at[:, pl.ds(pl.multiple_of(i * BN, BN), BN)], w_s.at[slot], w_sem.at[slot])

    for p in range(parts):
        x_copy(p).start()
    w_copy(wk_ref, 0, 0).start()
    w_copy(wk_ref, 1, 1).start()
    _greet(me, (1, 2, 3))

    moves = _transfers(groups)

    def move(n):
        src, dst, owner, first, wide, when = moves[n]
        here = kv_ref.at[pl.ds(owner * own, own), pl.ds(first, wide)]
        source = kv_s.at[:, pl.ds(first, wide)] if when < 2 else here
        return pltpu.make_async_remote_copy(source, here, send_sem.at[n], recv_sem.at[n], device_id={"sp": dst}, device_id_type=pl.DeviceIdType.MESH)

    def needed(n):
        src, dst, owner, first, wide, when = moves[n]
        return next(m for m, t in enumerate(moves) if t == (owner, src, owner, first, wide, when - 2))

    def launch(when):
        for n, t in enumerate(moves):
            if t[5] == when:

                @pl.when(me == t[0])
                def _():
                    if when >= 2:
                        move(needed(n)).wait_recv()
                    move(n).start()

    passed = {needed(n) for n, t in enumerate(moves) if t[5] >= 2}

    def norm(r, _):
        step = 16
        for b in range(2):
            at = pl.ds(pl.multiple_of((r * 2 + b) * step, step), step)
            wide = 512
            total = jnp.zeros((step, wide), F32)
            for c in range(0, depth, wide):
                t = a_s[at, c : c + wide].astype(F32)
                total += t * t
            scale = lax.rsqrt(jnp.sum(total, -1, keepdims=True) * (1 / depth) + 1e-6)
            for c in range(0, depth, wide):
                t = a_s[at, c : c + wide].astype(F32)
                a_s[at, c : c + wide] = (t * scale * gain_ref[:, c : c + wide]).astype(BF16)

    for p in range(parts):
        x_copy(p).wait()
        lax.fori_loop(p * rows // 32, (p + 1) * rows // 32, norm, None)

    def turn(acc, store):
        cos, sin = cos_ref[...], sin_ref[...]
        for at in range(0, BN, HEAD):
            t = acc[:, at : at + HEAD].astype(BF16).astype(F32)
            store(at, (t * cos + pltpu.roll(t, HEAD // 2, 1) * sin).astype(BF16))

    def keys(i, _):
        w_copy(wk_ref, i, i).wait()
        acc = _dot(a_s[...], w_s[i], 1, 0)
        w_copy(wv_ref, i, i).start()

        def store(at, t):
            kv_s[:, pl.ds(pl.multiple_of(i * BN + at, HEAD), HEAD)] = t

        turn(acc, store)

    lax.fori_loop(0, nk, keys, None)

    def values(i, _):
        w_copy(wv_ref, i, i).wait()
        acc = _dot(a_s[...], w_s[i], 1, 0)
        w_copy(wq_ref, i, i).start()
        kv_s[:, pl.ds(pl.multiple_of((nk + i) * BN, BN), BN)] = acc.astype(BF16)

        @pl.when(i == 0)
        def _():
            launch(0)

    lax.fori_loop(0, nk, values, None)

    def slot_of(i):
        return jnp.where(i < lots, i, lots + lax.rem(i, 2))

    def q_copy(i):
        slot = slot_of(i)
        return pltpu.make_async_copy(q_s.at[slot], q_ref.at[:, pl.ds(pl.multiple_of(i * BN, BN), BN)], q_sem.at[slot])

    def ship_copy(i):
        return pltpu.make_async_remote_copy(q_s.at[i], ship_ref.at[:, pl.ds(pl.multiple_of(i * BN, BN), BN)], ship_send.at[i], ship_recv.at[i],
                                            device_id={"sp": SP - 1 - me}, device_id_type=pl.DeviceIdType.MESH)

    gives = _by(me, SHIP) * per
    takes = _by(me, SHIP[::-1]) * per
    kv_out = pltpu.make_async_copy(kv_s, kv_ref.at[pl.ds(pl.multiple_of(me * own, own), own), :], kv_sem.at[0])

    def queries(i, _):
        slot = lax.rem(i, 2)
        w_copy(wq_ref, i, slot).wait()

        @pl.when(i >= lots + 2)
        def _():
            q_copy(i - 2).wait()

        acc = _dot(a_s[...], w_s[slot], 1, 0)

        @pl.when(i + 2 < nq)
        def _():
            w_copy(wq_ref, i + 2, slot).start()

        at_slot = slot_of(i)

        def store(at, t):
            q_s[at_slot, :, at : at + HEAD] = t

        turn(acc, store)
        q_copy(i).start()

        @pl.when((i >= 1) & (i - 1 < gives))
        def _():
            ship_copy(i - 1).start()

        @pl.when(i == 0)
        def _():
            launch(1)
            kv_out.start()

        @pl.when(i == 4)
        def _():
            launch(2)

        @pl.when(i == 7)
        def _():
            launch(3)

    lax.fori_loop(0, nq, queries, None)

    kv_out.wait()
    lax.fori_loop(0, lots, lambda i, _: q_copy(i).wait(), None)
    lax.fori_loop(nq - 2, nq, lambda i, _: q_copy(i).wait(), None)
    for n, t in enumerate(moves):

        @pl.when(me == t[0])
        def _():
            move(n).wait_send()

        if n not in passed:

            @pl.when(me == t[1])
            def _():
                move(n).wait_recv()

    lax.fori_loop(0, gives, lambda i, _: ship_copy(i).wait_send(), None)
    lax.fori_loop(0, takes, lambda i, _: ship_copy(i).wait_recv(), None)


def project(x, gain, wk, wv, wq, cos, sin):
    own, depth = x.shape
    width, both = wq.shape[1], wk.shape[1] + wv.shape[1]
    groups = wk.shape[1] // HEAD
    lots = MOST * (width // groups // BN)
    n = len(_transfers(groups))
    hbm, vmem = pl.BlockSpec(memory_space=pl.ANY), pl.BlockSpec(memory_space=pltpu.VMEM)
    dma = pltpu.SemaphoreType.DMA
    return pl.pallas_call(
        _project_kernel,
        in_specs=[hbm, vmem, hbm, hbm, hbm, vmem, vmem],
        out_specs=[hbm] * 3,
        out_shape=[jax.ShapeDtypeStruct((SP * own, both), BF16), jax.ShapeDtypeStruct((own, width), BF16),
                   jax.ShapeDtypeStruct((own, lots * BN), BF16)],
        scratch_shapes=[pltpu.VMEM((own, depth), BF16), pltpu.VMEM((2, depth, BN), BF16), pltpu.VMEM((own, both), BF16),
                        pltpu.VMEM((lots + 2, own, BN), BF16), dma((4,)), dma((2,)), dma((1,)), dma((lots + 2,)), dma((n,)), dma((n,)),
                        dma((lots,)), dma((lots,))],
        compiler_params=pltpu.CompilerParams(vmem_limit_bytes=VMEM, collective_id=0, has_side_effects=True),
        cost_estimate=pl.CostEstimate(flops=2 * own * depth * (width + both), transcendentals=own, bytes_accessed=2 * depth * (width + both)),
    )(x, gain.astype(F32).reshape(1, depth), wk, wv, wq, cos, sin)


def _attend_kernel(q_ref, ship_ref, kv_ref, wo_ref, x_ref, y_ref, q_s, k_s, v_s, o_s, give_s, top_s, mix_s, w_s, acc_s, x_s, y_s,
                   q_sem, k_sem, v_sem, w_sem, x_sem, y_sem, send_sem, recv_sem):
    me = lax.axis_index("sp")
    own, width = q_ref.shape
    groups = kv_ref.shape[1] // (2 * HEAD)
    g = width // groups
    heads = g // HEAD
    n_out = wo_ref.shape[1] // BN
    few = MOST * g
    e = HEAD**-0.5 * LOG2E
    gives, takes = _by(me, SHIP), _by(me, SHIP[::-1])
    jobs = takes + groups - gives

    def w_copy(i, slot):
        below = wo_ref.shape[0] - few
        later = i >= n_out

        def rows(first, count, block):
            cols = pl.ds(pl.multiple_of(block * BN, BN), BN)
            return pltpu.make_async_copy(wo_ref.at[pl.ds(first, count), cols], w_s.at[slot, pl.ds(0, count), :], w_sem.at[slot])

        return rows(few, below, i), rows(0, few, i - n_out), later

    def w_start(i, slot):
        first, second, later = w_copy(i, slot)
        pl.when(jnp.logical_not(later))(lambda: first.start())
        pl.when(later)(lambda: second.start())

    w_start(jnp.int32(0), 0)
    w_start(jnp.int32(1), 1)

    def job(j):
        given = j < takes
        return given, jnp.where(given, j, gives + j - takes), jnp.where(given, SP - 1 - me, me)

    def fetch(j, slot, wait):
        given, head, at = job(j)
        cols = pl.ds(pl.multiple_of(head * g, g), g)
        here, there = (pltpu.make_async_copy(ref.at[:, cols], q_s.at[slot], q_sem.at[slot]) for ref in (q_ref, ship_ref))
        if wait:
            here.wait()
        else:
            pl.when(given)(lambda: there.start())
            pl.when(jnp.logical_not(given))(lambda: here.start())
        for b in range(SP):
            rows = pl.ds(b * own, own)
            for ref, sem, first in ((k_s, k_sem, 0), (v_s, v_sem, groups)):
                copy = pltpu.make_async_copy(kv_ref.at[rows, pl.ds(pl.multiple_of((first + head) * HEAD, HEAD), HEAD)], ref.at[slot, rows, :],
                                             sem.at[slot, b])
                pl.when(b <= at)(lambda: copy.wait() if wait else copy.start())

    fetch(jnp.int32(0), 0, False)
    barrier = pltpu.get_barrier_semaphore()
    pl.semaphore_signal(barrier, inc=1, device_id={"sp": SP - 1 - me}, device_id_type=pl.DeviceIdType.MESH)
    pl.semaphore_wait(barrier, 1)

    def give(i):
        return pltpu.make_async_remote_copy(give_s.at[i], o_s.at[:, pl.ds(pl.multiple_of(i * g, g), g)], send_sem.at[i], recv_sem.at[i],
                                            device_id={"sp": SP - 1 - me}, device_id_type=pl.DeviceIdType.MESH)

    def attend(j, _):
        slot = lax.rem(j, 2)
        given, head, at = job(j)

        @pl.when(j + 1 < jobs)
        def _():
            fetch(j + 1, 1 - slot, False)

        fetch(j, slot, True)
        top_s[...] = jnp.full(top_s.shape, NEG, F32)
        mix_s[...] = jnp.zeros(mix_s.shape, F32)

        def block(first, keys, cols, wide, masked):
            here = pl.ds(first, keys)
            k, values = k_s[slot, here, :], jnp.concatenate([v_s[slot, here, :].T, jnp.ones((8, keys), BF16)], axis=0)
            scores = [_dot(k, q_s[slot, cols : cols + wide, h * HEAD : (h + 1) * HEAD], 1, 1) for h in range(heads)]
            if masked:
                shape = (keys, wide)
                ok = lax.broadcasted_iota(jnp.int32, shape, 0) <= lax.broadcasted_iota(jnp.int32, shape, 1) + cols
            weights, keeps = [], []
            for h, s in enumerate(scores):
                if masked:
                    s = jnp.where(ok, s, HIDDEN)
                old = top_s[h : h + 1, cols : cols + wide]
                top = jnp.maximum(old, s.max(axis=0, keepdims=True))
                top_s[h : h + 1, cols : cols + wide] = top
                weights.append(jnp.exp2((s - top) * e).astype(BF16))
                keeps.append(jnp.exp2((old - top) * e))
            for h in range(heads):
                mix_s[h, :, cols : cols + wide] = mix_s[h, :, cols : cols + wide] * keeps[h] + _dot(values, weights[h], 1, 0)

        lax.fori_loop(0, at, lambda b, _: block(pl.multiple_of(b * own, own), own, 0, own, False), None)
        here = pl.multiple_of(at * own, own)
        half = own // 2
        block(here, half, 0, half, True)
        block(here, own, half, half, True)

        def result(h):
            return (mix_s[h, :HEAD, :] * (1 / mix_s[h, HEAD : HEAD + 1, :])).T.astype(BF16)

        @pl.when(given)
        def _():
            for h in range(heads):
                give_s[head, :, h * HEAD : (h + 1) * HEAD] = result(h)

        @pl.when(jnp.logical_not(given))
        def _():
            for h in range(heads):
                o_s[:, pl.ds(pl.multiple_of(head * g + h * HEAD, HEAD), HEAD)] = result(h)

        @pl.when((j >= 1) & (j - 1 < takes))
        def _():
            give(j - 1).start()

    lax.fori_loop(0, jobs, attend, None)

    def first_part(i, _):
        slot = lax.rem(i, 2)
        w_copy(i, slot)[0].wait()
        acc_s[i] = _dot(o_s[:, few:], w_s[slot], 1, 0)
        w_start(i + 2, slot)

    lax.fori_loop(0, n_out, first_part, None)

    def x_copy(i, slot):
        return pltpu.make_async_copy(x_ref.at[:, pl.ds(pl.multiple_of(i * BN, BN), BN)], x_s.at[slot], x_sem.at[slot])

    def y_copy(i, slot):
        return pltpu.make_async_copy(y_s.at[slot], y_ref.at[:, pl.ds(pl.multiple_of(i * BN, BN), BN)], y_sem.at[slot])

    x_copy(0, 0).start()
    x_copy(1, 1).start()
    lax.fori_loop(0, gives, lambda i, _: give(i).wait_recv(), None)

    def second_part(i, _):
        slot = lax.rem(i, 2)
        w_copy(i + n_out, slot)[1].wait()
        x_copy(i, slot).wait()

        @pl.when(i >= 2)
        def _():
            y_copy(i - 2, slot).wait()

        acc = acc_s[i] + _dot(o_s[:, :few], w_s[slot, :few, :], 1, 0)
        y_s[slot] = (x_s[slot].astype(F32) + acc).astype(BF16)
        y_copy(i, slot).start()

        @pl.when(i + 2 < n_out)
        def _():
            w_copy(i + 2 + n_out, slot)[1].start()
            x_copy(i + 2, slot).start()

    lax.fori_loop(0, n_out, second_part, None)
    y_copy(n_out - 2, (n_out - 2) % 2).wait()
    y_copy(n_out - 1, (n_out - 1) % 2).wait()
    lax.fori_loop(0, takes, lambda i, _: give(i).wait_send(), None)


def attend_out(q, ship, kv, wo, x):
    own, width = q.shape
    rows, groups = kv.shape[0], kv.shape[1] // (2 * HEAD)
    g = width // groups
    n_out = wo.shape[1] // BN
    hbm = pl.BlockSpec(memory_space=pl.ANY)
    dma = pltpu.SemaphoreType.DMA
    return pl.pallas_call(
        _attend_kernel,
        in_specs=[hbm] * 5,
        out_specs=hbm,
        out_shape=jax.ShapeDtypeStruct(x.shape, BF16),
        scratch_shapes=[
            pltpu.VMEM((2, own, g), BF16), pltpu.VMEM((2, rows, HEAD), BF16), pltpu.VMEM((2, rows, HEAD), BF16), pltpu.VMEM((own, width), BF16),
            pltpu.VMEM((MOST, own, g), BF16), pltpu.VMEM((g // HEAD, own), F32), pltpu.VMEM((g // HEAD, HEAD + 8, own), F32),
            pltpu.VMEM((2, width - MOST * g, BN), BF16), pltpu.VMEM((n_out, own, BN), F32), pltpu.VMEM((2, own, BN), BF16),
            pltpu.VMEM((2, own, BN), BF16), dma((2,)), dma((2, SP)), dma((2, SP)), dma((2,)), dma((2,)), dma((2,)), dma((MOST,)), dma((MOST,)),
        ],
        compiler_params=pltpu.CompilerParams(vmem_limit_bytes=VMEM, collective_id=1, has_side_effects=True),
        cost_estimate=pl.CostEstimate(flops=2 * own * width * (rows + wo.shape[1]), transcendentals=own * rows * width // HEAD, bytes_accessed=2 * wo.size),
    )(q, ship, kv, wo, x)


def tables(place):
    half = HEAD // 2
    angle = place.astype(F32)[:, None] * THETA ** (-jnp.arange(half, dtype=F32) / half)
    cos, sin = jnp.cos(angle), jnp.sin(angle)
    return jnp.concatenate([cos, cos], -1), jnp.concatenate([-sin, sin], -1)


def solution(mesh):
    def step(x, gain, wq, wk, wv, wo):
        own = x.shape[0]
        cos, sin = tables(lax.axis_index("sp") * own + jnp.arange(own))
        kv, q, ship = project(x, gain, wk, wv, wq, cos, sin)
        return attend_out(q, ship, kv, wo, x)

    tokens, whole = P(("dp", "sp"), None), P(None, None)
    return jax.shard_map(
        step,
        mesh=mesh,
        in_specs=(tokens, P(None), whole, whole, whole, whole),
        out_specs=tokens,
        check_vma=False,
    )
```

```python
import functools

import jax
import jax.numpy as jnp
from jax import lax
from jax.experimental import pallas as pl
from jax.experimental.pallas import tpu as pltpu
from jax.sharding import PartitionSpec as P

HEAD = 128
THETA = 10000
NEG = -1e30
HIDDEN = 2 * NEG
LOG2E = 1.4426950408889634
VMEM = 63 * 2**20
F32, BF16 = jnp.float32, jnp.bfloat16
SP = 4
SHIP = (0, 0, 1, 3)
MOST = max(SHIP)
BN = 512
EARLY = 8


def _dot(a, b, ca, cb):
    return lax.dot_general(a, b, (((ca,), (cb,)), ((), ())), preferred_element_type=F32)


def _by(me, values):
    out = jnp.int32(values[0])
    for s, v in enumerate(values[1:], 1):
        out = jnp.where(me == s, jnp.int32(v), out)
    return out


def _greet(me, others):
    barrier = pltpu.get_barrier_semaphore()
    for d in others:
        pl.semaphore_signal(barrier, inc=1, device_id={"sp": lax.rem(me + d, SP)}, device_id_type=pl.DeviceIdType.MESH)
    pl.semaphore_wait(barrier, len(others))


def _transfers(groups):
    s, whole = MOST * HEAD, groups * HEAD
    out = []
    for v in range(2):
        few, rest = (v * whole, s), (v * whole + s, whole - s)
        for src, dst, cols in ((0, 1, few), (0, 1, rest), (0, 3, rest), (1, 2, rest), (1, 2, few), (1, 0, few), (2, 3, rest), (2, 1, few), (3, 0, few)):
            out.append((src, dst, src, *cols, v))
        for src, dst, owner, cols in ((1, 2, 0, few), (3, 2, 0, rest), (2, 3, 1, rest), (1, 0, 2, few)):
            out.append((src, dst, owner, *cols, 2 + v))
    return out


def _project_kernel(x_ref, gain_ref, wk_ref, wv_ref, wq_ref, cos_ref, sin_ref, kv_ref, q_ref, ship_ref,
                    a_s, w_s, kv_s, q_s, cos_s, sin_s, x_sem, w_sem, kv_sem, q_sem, send_sem, recv_sem, ship_send, ship_recv):
    me = lax.axis_index("sp")
    own, depth = a_s.shape
    groups = wk_ref.shape[1] // HEAD
    nk, nq = wk_ref.shape[1] // BN, wq_ref.shape[1] // BN
    per = wq_ref.shape[1] // groups // BN
    lots = MOST * per
    parts = 4
    rows = own // parts

    def x_copy(p):
        at = pl.ds(p * rows, rows)
        return pltpu.make_async_copy(x_ref.at[at, :], a_s.at[at, :], x_sem.at[p])

    def w_copy(ref, i, slot):
        return pltpu.make_async_copy(ref.at[:, pl.ds(pl.multiple_of(i * BN, BN), BN)], w_s.at[slot], w_sem.at[slot])

    for p in range(parts):
        x_copy(p).start()
    w_copy(wk_ref, 0, 0).start()
    w_copy(wk_ref, 1, 1).start()
    _greet(me, (1, 2, 3))

    moves = _transfers(groups)

    def move(n):
        src, dst, owner, first, wide, when = moves[n]
        here = kv_ref.at[pl.ds(owner * own, own), pl.ds(first, wide)]
        source = kv_s.at[:, pl.ds(first, wide)] if when < 2 else here
        return pltpu.make_async_remote_copy(source, here, send_sem.at[n], recv_sem.at[n], device_id={"sp": dst}, device_id_type=pl.DeviceIdType.MESH)

    def needed(n):
        src, dst, owner, first, wide, when = moves[n]
        return next(m for m, t in enumerate(moves) if t == (owner, src, owner, first, wide, when - 2))

    def launch(when):
        for n, t in enumerate(moves):
            if t[5] == when:

                @pl.when(me == t[0])
                def _():
                    if when >= 2:
                        move(needed(n)).wait_recv()
                    move(n).start()

    passed = {needed(n) for n, t in enumerate(moves) if t[5] >= 2}

    def norm(r, _):
        step = 16
        for b in range(2):
            at = pl.ds(pl.multiple_of((r * 2 + b) * step, step), step)
            wide = 512
            total = jnp.zeros((step, wide), F32)
            for c in range(0, depth, wide):
                t = a_s[at, c : c + wide].astype(F32)
                total += t * t
            scale = lax.rsqrt(jnp.sum(total, -1, keepdims=True) * (1 / depth) + 1e-6)
            for c in range(0, depth, wide):
                t = a_s[at, c : c + wide].astype(F32)
                a_s[at, c : c + wide] = (t * scale * gain_ref[:, c : c + wide]).astype(BF16)

    for p in range(parts):
        x_copy(p).wait()
        lax.fori_loop(p * rows // 32, (p + 1) * rows // 32, norm, None)

    cos_s[...] = jnp.concatenate([cos_ref[...], cos_ref[...]], -1)
    sin_s[...] = jnp.concatenate([-sin_ref[...], sin_ref[...]], -1)

    def turn(acc, store):
        cos, sin = cos_s[...], sin_s[...]
        for at in range(0, BN, HEAD):
            t = acc[:, at : at + HEAD].astype(BF16).astype(F32)
            store(at, (t * cos + pltpu.roll(t, HEAD // 2, 1) * sin).astype(BF16))

    def keys(i, _):
        w_copy(wk_ref, i, i).wait()
        acc = _dot(a_s[...], w_s[i], 1, 0)
        w_copy(wq_ref, i, i).start()

        def store(at, t):
            kv_s[:, pl.ds(pl.multiple_of(i * BN + at, HEAD), HEAD)] = t

        turn(acc, store)

        @pl.when(i == nk - 1)
        def _():
            launch(0)

    lax.fori_loop(0, nk, keys, None)

    def slot_of(i):
        return jnp.where(i < lots, i, lots + lax.rem(i, 2))

    def q_copy(i):
        slot = slot_of(i)
        return pltpu.make_async_copy(q_s.at[slot], q_ref.at[:, pl.ds(pl.multiple_of(i * BN, BN), BN)], q_sem.at[slot])

    def ship_copy(i):
        return pltpu.make_async_remote_copy(q_s.at[i], ship_ref.at[:, pl.ds(pl.multiple_of(i * BN, BN), BN)], ship_send.at[i], ship_recv.at[i],
                                            device_id={"sp": SP - 1 - me}, device_id_type=pl.DeviceIdType.MESH)

    gives = _by(me, SHIP) * per
    takes = _by(me, SHIP[::-1]) * per
    kv_out = pltpu.make_async_copy(kv_s, kv_ref.at[pl.ds(pl.multiple_of(me * own, own), own), :], kv_sem.at[0])

    def queries(i, _):
        slot = lax.rem(i, 2)
        w_copy(wq_ref, i, slot).wait()

        @pl.when(i >= lots + 2)
        def _():
            q_copy(i - 2).wait()

        acc = _dot(a_s[...], w_s[slot], 1, 0)

        @pl.when(i < nk)
        def _():
            w_copy(wv_ref, i, slot).start()

        @pl.when((i >= nk) & (i + 2 < nq))
        def _():
            w_copy(wq_ref, i + 2, slot).start()

        at_slot = slot_of(i)

        def store(at, t):
            q_s[at_slot, :, at : at + HEAD] = t

        turn(acc, store)
        q_copy(i).start()

        @pl.when(i < gives)
        def _():
            ship_copy(i).start()

        @pl.when(i == nk + 1)
        def _():
            launch(2)

        @pl.when(i == nk + 4)
        def _():
            launch(3)

    def values(i, _):
        w_copy(wv_ref, i, i).wait()
        acc = _dot(a_s[...], w_s[i], 1, 0)
        w_copy(wq_ref, nk + i, i).start()
        kv_s[:, pl.ds(pl.multiple_of((nk + i) * BN, BN), BN)] = acc.astype(BF16)

        @pl.when(i == nk - 1)
        def _():
            launch(1)
            kv_out.start()

    lax.fori_loop(0, nk, queries, None)
    lax.fori_loop(0, nk, values, None)
    lax.fori_loop(nk, nq, queries, None)

    kv_out.wait()
    lax.fori_loop(0, lots, lambda i, _: q_copy(i).wait(), None)
    lax.fori_loop(nq - 2, nq, lambda i, _: q_copy(i).wait(), None)
    for n, t in enumerate(moves):

        @pl.when(me == t[0])
        def _():
            move(n).wait_send()

        if n not in passed:

            @pl.when(me == t[1])
            def _():
                move(n).wait_recv()

    lax.fori_loop(0, gives, lambda i, _: ship_copy(i).wait_send(), None)
    lax.fori_loop(0, takes, lambda i, _: ship_copy(i).wait_recv(), None)


def project(x, gain, wk, wv, wq, cos, sin):
    own, depth = x.shape
    width, both = wq.shape[1], wk.shape[1] + wv.shape[1]
    groups = wk.shape[1] // HEAD
    lots = MOST * (width // groups // BN)
    n = len(_transfers(groups))
    hbm, vmem = pl.BlockSpec(memory_space=pl.ANY), pl.BlockSpec(memory_space=pltpu.VMEM)
    dma = pltpu.SemaphoreType.DMA
    return pl.pallas_call(
        _project_kernel,
        in_specs=[hbm, vmem, hbm, hbm, hbm, vmem, vmem],
        out_specs=[hbm] * 3,
        out_shape=[jax.ShapeDtypeStruct((SP * own, both), BF16), jax.ShapeDtypeStruct((own, width), BF16),
                   jax.ShapeDtypeStruct((own, lots * BN), BF16)],
        scratch_shapes=[pltpu.VMEM((own, depth), BF16), pltpu.VMEM((2, depth, BN), BF16), pltpu.VMEM((own, both), BF16),
                        pltpu.VMEM((lots + 2, own, BN), BF16), pltpu.VMEM((own, HEAD), F32), pltpu.VMEM((own, HEAD), F32), dma((4,)), dma((2,)), dma((1,)), dma((lots + 2,)), dma((n,)), dma((n,)),
                        dma((lots,)), dma((lots,))],
        compiler_params=pltpu.CompilerParams(vmem_limit_bytes=VMEM, collective_id=0, has_side_effects=True),
        cost_estimate=pl.CostEstimate(flops=2 * own * depth * (width + both), transcendentals=own, bytes_accessed=2 * depth * (width + both)),
    )(x, gain.astype(F32).reshape(1, depth), wk, wv, wq, cos, sin)


def _attend_kernel(q_ref, ship_ref, kv_ref, wo_ref, part_ref, seen_ref, q_s, k_s, v_s, o_s, give_s, top_s, mix_s, w_s, part_s,
                   q_sem, k_sem, v_sem, w_sem, part_sem, seen_sem, send_sem, recv_sem):
    me = lax.axis_index("sp")
    own, width = q_ref.shape
    groups = kv_ref.shape[1] // (2 * HEAD)
    g = width // groups
    heads = g // HEAD
    few = MOST * g
    e = HEAD**-0.5 * LOG2E
    gives, takes = _by(me, SHIP), _by(me, SHIP[::-1])
    jobs = takes + groups - gives

    def w_copy(i, slot):
        cols = pl.ds(pl.multiple_of(i * BN, BN), BN)
        return pltpu.make_async_copy(wo_ref.at[pl.ds(few, wo_ref.shape[0] - few), cols], w_s.at[slot], w_sem.at[slot])

    w_copy(0, 0).start()
    w_copy(1, 1).start()

    def job(j):
        given = j < takes
        return given, jnp.where(given, j, gives + j - takes), jnp.where(given, SP - 1 - me, me)

    def fetch(j, slot, wait):
        given, head, at = job(j)
        cols = pl.ds(pl.multiple_of(head * g, g), g)
        here, there = (pltpu.make_async_copy(ref.at[:, cols], q_s.at[slot], q_sem.at[slot]) for ref in (q_ref, ship_ref))
        if wait:
            here.wait()
        else:
            pl.when(given)(lambda: there.start())
            pl.when(jnp.logical_not(given))(lambda: here.start())
        for b in range(SP):
            rows = pl.ds(b * own, own)
            for ref, sem, first in ((k_s, k_sem, 0), (v_s, v_sem, groups)):
                copy = pltpu.make_async_copy(kv_ref.at[rows, pl.ds(pl.multiple_of((first + head) * HEAD, HEAD), HEAD)], ref.at[slot, rows, :],
                                             sem.at[slot, b])
                pl.when(b <= at)(lambda: copy.wait() if wait else copy.start())

    fetch(jnp.int32(0), 0, False)
    barrier = pltpu.get_barrier_semaphore()
    pl.semaphore_signal(barrier, inc=1, device_id={"sp": SP - 1 - me}, device_id_type=pl.DeviceIdType.MESH)
    pl.semaphore_wait(barrier, 1)

    def give(i):
        return pltpu.make_async_remote_copy(give_s.at[i], o_s.at[:, pl.ds(pl.multiple_of(i * g, g), g)], send_sem.at[i], recv_sem.at[i],
                                            device_id={"sp": SP - 1 - me}, device_id_type=pl.DeviceIdType.MESH)

    def seen_copy(head):
        cols = pl.ds(pl.multiple_of(head * g, g), g)
        return pltpu.make_async_copy(o_s.at[:, cols], seen_ref.at[:, cols], seen_sem.at[head])

    def attend(j, _):
        slot = lax.rem(j, 2)
        given, head, at = job(j)

        @pl.when(j + 1 < jobs)
        def _():
            fetch(j + 1, 1 - slot, False)

        fetch(j, slot, True)
        top_s[...] = jnp.full(top_s.shape, NEG, F32)
        mix_s[...] = jnp.zeros(mix_s.shape, F32)

        def block(first, keys, cols, wide, masked):
            here = pl.ds(first, keys)
            k, values = k_s[slot, here, :], jnp.concatenate([v_s[slot, here, :].T, jnp.ones((8, keys), BF16)], axis=0)
            scores = [_dot(k, q_s[slot, cols : cols + wide, h * HEAD : (h + 1) * HEAD], 1, 1) for h in range(heads)]
            if masked:
                shape = (keys, wide)
                ok = lax.broadcasted_iota(jnp.int32, shape, 0) <= lax.broadcasted_iota(jnp.int32, shape, 1) + cols
            weights, keeps = [], []
            for h, s in enumerate(scores):
                if masked:
                    s = jnp.where(ok, s, HIDDEN)
                old = top_s[h : h + 1, cols : cols + wide]
                top = jnp.maximum(old, s.max(axis=0, keepdims=True))
                top_s[h : h + 1, cols : cols + wide] = top
                weights.append(jnp.exp2((s - top) * e).astype(BF16))
                keeps.append(jnp.exp2((old - top) * e))
            for h in range(heads):
                mix_s[h, :, cols : cols + wide] = mix_s[h, :, cols : cols + wide] * keeps[h] + _dot(values, weights[h], 1, 0)

        lax.fori_loop(0, at, lambda b, _: block(pl.multiple_of(b * own, own), own, 0, own, False), None)
        here = pl.multiple_of(at * own, own)
        half = own // 2
        block(here, half, 0, half, True)
        block(here, own, half, half, True)

        def result(h):
            return (mix_s[h, :HEAD, :] * (1 / mix_s[h, HEAD : HEAD + 1, :])).T.astype(BF16)

        @pl.when(given)
        def _():
            for h in range(heads):
                give_s[head, :, h * HEAD : (h + 1) * HEAD] = result(h)

        @pl.when(jnp.logical_not(given))
        def _():
            for h in range(heads):
                o_s[:, pl.ds(pl.multiple_of(head * g + h * HEAD, HEAD), HEAD)] = result(h)
            seen_copy(head).start()

        @pl.when(given)
        def _():
            give(j).start()

    lax.fori_loop(0, jobs, attend, None)

    def part_copy(i, slot):
        return pltpu.make_async_copy(part_s.at[slot], part_ref.at[:, pl.ds(pl.multiple_of(i * BN, BN), BN)], part_sem.at[slot])

    def first_part(i, _):
        slot = lax.rem(i, 2)
        w_copy(i, slot).wait()

        @pl.when(i >= 2)
        def _():
            part_copy(i - 2, slot).wait()

        part_s[slot] = _dot(o_s[:, few:], w_s[slot], 1, 0)
        part_copy(i, slot).start()

        @pl.when(i + 2 < EARLY)
        def _():
            w_copy(i + 2, slot).start()

    lax.fori_loop(0, EARLY, first_part, None)

    def received(i, _):
        give(i).wait_recv()
        seen_copy(i).start()

    lax.fori_loop(0, gives, received, None)
    part_copy(EARLY - 2, EARLY % 2).wait()
    part_copy(EARLY - 1, (EARLY - 1) % 2).wait()
    lax.fori_loop(0, takes, lambda i, _: give(i).wait_send(), None)
    lax.fori_loop(0, groups, lambda i, _: seen_copy(i).wait(), None)


def attend(q, ship, kv, wo):
    own, width = q.shape
    rows, groups = kv.shape[0], kv.shape[1] // (2 * HEAD)
    g = width // groups
    few = MOST * g
    hbm = pl.BlockSpec(memory_space=pl.ANY)
    dma = pltpu.SemaphoreType.DMA
    return pl.pallas_call(
        _attend_kernel,
        in_specs=[hbm] * 4,
        out_specs=[hbm] * 2,
        out_shape=[jax.ShapeDtypeStruct((own, EARLY * BN), F32), jax.ShapeDtypeStruct((own, width), BF16)],
        scratch_shapes=[
            pltpu.VMEM((2, own, g), BF16), pltpu.VMEM((2, rows, HEAD), BF16), pltpu.VMEM((2, rows, HEAD), BF16), pltpu.VMEM((own, width), BF16),
            pltpu.VMEM((MOST, own, g), BF16), pltpu.VMEM((g // HEAD, own), F32), pltpu.VMEM((g // HEAD, HEAD + 8, own), F32),
            pltpu.VMEM((2, width - few, BN), BF16), pltpu.VMEM((2, own, BN), F32),
            dma((2,)), dma((2, SP)), dma((2, SP)), dma((2,)), dma((2,)), dma((groups,)), dma((MOST,)), dma((MOST,)),
        ],
        compiler_params=pltpu.CompilerParams(vmem_limit_bytes=VMEM, collective_id=1, has_side_effects=True),
        cost_estimate=pl.CostEstimate(flops=2 * own * width * (rows + wo.shape[1]), transcendentals=own * rows * width // HEAD, bytes_accessed=2 * wo.size),
    )(q, ship, kv, wo)


def _finish_kernel(few, seen_ref, wo_ref, part_ref, x_ref, y_ref, seen_s, w_s, part_s, x_s, y_s, seen_sem, w_sem, part_sem, x_sem, y_sem):
    below = seen_s.shape[1] - few
    n_out = wo_ref.shape[1] // BN

    def cols(i):
        return pl.ds(pl.multiple_of(i * BN, BN), BN)

    def seen_copy(n, first, count):
        return pltpu.make_async_copy(seen_ref.at[:, pl.ds(first, count)], seen_s.at[:, pl.ds(first, count)], seen_sem.at[n])

    def w_copy(i, slot, rows):
        return pltpu.make_async_copy(wo_ref.at[pl.ds(0, rows), cols(i)], w_s.at[slot, pl.ds(0, rows), :], w_sem.at[slot])

    def part_copy(i, slot):
        return pltpu.make_async_copy(part_ref.at[:, cols(i)], part_s.at[slot], part_sem.at[slot])

    def x_copy(i, slot):
        return pltpu.make_async_copy(x_ref.at[:, cols(i)], x_s.at[slot], x_sem.at[slot])

    def y_copy(i, slot):
        return pltpu.make_async_copy(y_s.at[slot], y_ref.at[:, cols(i)], y_sem.at[slot])

    seen_copy(0, 0, few).start()
    for i in range(2):
        w_copy(i, i, few).start()
        part_copy(i, i).start()
        x_copy(i, i).start()
    seen_copy(0, 0, few).wait()

    def step(i, early):
        slot = lax.rem(i, 2)
        rows = few if early else few + below
        w_copy(i, slot, rows).wait()
        x_copy(i, slot).wait()

        @pl.when(i >= 2)
        def _():
            y_copy(i - 2, slot).wait()

        acc = _dot(seen_s[:, :rows], w_s[slot, :rows, :], 1, 0)
        if early:
            part_copy(i, slot).wait()
            acc += part_s[slot]
        y_s[slot] = (x_s[slot].astype(F32) + acc).astype(BF16)
        y_copy(i, slot).start()

        @pl.when(i + 2 < n_out)
        def _():
            x_copy(i + 2, slot).start()

        if early:

            @pl.when(i + 2 < EARLY)
            def _():
                part_copy(i + 2, slot).start()
                w_copy(i + 2, slot, few).start()

            @pl.when(i + 2 >= EARLY)
            def _():
                w_copy(i + 2, slot, few + below).start()

            @pl.when(i == 1)
            def _():
                seen_copy(1, few, below).start()

        else:

            @pl.when(i + 2 < n_out)
            def _():
                w_copy(i + 2, slot, few + below).start()

    lax.fori_loop(0, EARLY, lambda i, _: step(i, True), None)
    seen_copy(1, few, below).wait()
    lax.fori_loop(EARLY, n_out, lambda i, _: step(i, False), None)
    y_copy(n_out - 2, n_out % 2).wait()
    y_copy(n_out - 1, (n_out - 1) % 2).wait()


def finish(seen, wo, part, x, few):
    own, width = seen.shape
    hbm = pl.BlockSpec(memory_space=pl.ANY)
    dma = pltpu.SemaphoreType.DMA
    return pl.pallas_call(
        functools.partial(_finish_kernel, few),
        in_specs=[hbm] * 4,
        out_specs=hbm,
        out_shape=jax.ShapeDtypeStruct(x.shape, BF16),
        scratch_shapes=[
            pltpu.VMEM((own, width), BF16), pltpu.VMEM((2, width, BN), BF16), pltpu.VMEM((2, own, BN), F32), pltpu.VMEM((2, own, BN), BF16),
            pltpu.VMEM((2, own, BN), BF16), dma((2,)), dma((2,)), dma((2,)), dma((2,)), dma((2,)),
        ],
        compiler_params=pltpu.CompilerParams(vmem_limit_bytes=VMEM),
        cost_estimate=pl.CostEstimate(flops=2 * own * few * wo.shape[1], transcendentals=0, bytes_accessed=2 * few * wo.shape[1] + 8 * x.size),
    )(seen, wo, part, x)


def tables(place):
    half = HEAD // 2
    angle = place.astype(F32)[:, None] * THETA ** (-jnp.arange(half, dtype=F32) / half)
    return jnp.cos(angle), jnp.sin(angle)


def solution(mesh):
    def step(x, gain, wq, wk, wv, wo):
        own = x.shape[0]
        cos, sin = tables(lax.axis_index("sp") * own + jnp.arange(own))
        kv, q, ship = project(x, gain, wk, wv, wq, cos, sin)
        part, seen = attend(q, ship, kv, wo)
        return finish(seen, wo, part, x, MOST * wq.shape[1] // (wk.shape[1] // HEAD))

    tokens, whole = P(("dp", "sp"), None), P(None, None)
    return jax.shard_map(
        step,
        mesh=mesh,
        in_specs=(tokens, P(None), whole, whole, whole, whole),
        out_specs=tokens,
        check_vma=False,
    )
```
